32 devices in a mesh: db: 8 (over z, y), sub: 4 (over x, core).
Axes of the slice: x: 2, y: 2, z: 4, core: 2. Of those that a mesh axis runs over, the one named last changes fastest.
Arguments:
- codes: int32 [8192, 64], P('db', 'sub'), may hold values from 0 to 255
- tables: bfloat16 [512, 64, 256], P('db', 'sub'), may hold values from 0.125 to 128, as said below
- limits: int32 [512], replicated, may hold values from 3008 to 3263
Outputs:
- hit_ids: int32 [512, 128], P(('db', 'sub'))
- hit_count: int32 [512], P(('db', 'sub'))
The draws below stay inside these ranges and needn't reach their ends.
Inputs may be any that keep to these rules, and one draw needn't show every extreme that they name: `tables`: each value is a bfloat16 number of at least 1/8 and at most 128.
All inputs are finite; a program needn't handle non-finite values.
Results may differ from the reference program's by a relative error of at most 0.000001.
Values may be sent and summed in bfloat16 or wider, within the bound.
A program may use at most 128 MiB of HBM per device.

```python
import jax
import jax.numpy as jnp
from jax import lax

M = 64
K = 256
SLOTS = 128
ROWS = 1024
Q = 512
DB_ROWS = 8192


def nearest_centroids(key):
    return jax.random.randint(jax.random.fold_in(key, 7101), (Q, M), 0, K, dtype=jnp.int32)


def draw_tables(key, part):
    nearest = nearest_centroids(key)
    drawn = jax.random.uniform(jax.random.fold_in(key, 7201), (Q, M, K), jnp.float32, 0.125, 128.0)
    lowered = jax.random.uniform(jax.random.fold_in(key, 7204), (Q, M, K), jnp.float32, 0.125, 80.0)
    heavy = jax.random.randint(jax.random.fold_in(key, 7203), (Q,), 0, 8, dtype=jnp.int32) == 0
    values = jnp.where(heavy[:, None, None], lowered, drawn)
    lowest = jax.random.uniform(jax.random.fold_in(key, 7202), (Q, M), jnp.float32, 0.125, 16.0)
    centroid = lax.iota(jnp.int32, K)
    chosen = centroid[None, None, :] == nearest[:, :, None]
    return jnp.where(chosen, lowest[:, :, None], values).astype(jnp.bfloat16)


def draw_codes(key, part):
    nearest = nearest_centroids(key)
    ranges = DB_ROWS // ROWS
    planted_count = SLOTS + SLOTS // 2
    base = jax.random.randint(jax.random.fold_in(key, 7301), (DB_ROWS, M), 0, K, dtype=jnp.int32)
    target = jax.random.randint(jax.random.fold_in(key, 7302), (ranges,), 0, Q, dtype=jnp.int32)
    range_keys = jax.random.split(jax.random.fold_in(key, 7303), ranges)
    ranks = jax.vmap(lambda one_key: jax.random.permutation(one_key, ROWS))(range_keys)
    planted = (ranks < planted_count).reshape(DB_ROWS)
    offset = jax.random.randint(jax.random.fold_in(key, 7304), (DB_ROWS,), 0, 4, dtype=jnp.int32)
    subspace = lax.iota(jnp.int32, M)
    copied = planted[:, None] & ((subspace[None, :] + offset[:, None]) % 4 != 0)
    near_rows = jnp.repeat(nearest[target], ROWS, axis=0)
    return jnp.where(copied, near_rows, base).astype(jnp.int32)


def plant(values, own_key, smallest, top_value):
    extent = values.shape
    spot = [jax.random.randint(jax.random.fold_in(own_key, axis), (), 0, extent[axis]) for axis in range(len(extent))]
    values = values.at[tuple(spot)].set(smallest)
    longest = extent.index(max(extent))
    spot[longest] = (spot[longest] + 1) % extent[longest]
    return values.at[tuple(spot)].set(top_value)


def setup_inputs(seed: int = 0) -> dict:
    splits = jax.random.split(jax.random.key(seed), 4)
    codes = draw_codes(jax.random.fold_in(splits[3], 71), 0)
    tables = draw_tables(jax.random.fold_in(splits[3], 71), 0)
    limits = plant(jax.random.randint(splits[2], (Q,), M * 47, M * 51), jax.random.fold_in(splits[2], 1), M * 47, (M * 51) - 1).astype(jnp.int32)
    return dict(codes=codes, tables=tables, limits=limits)


def reference(codes, tables, limits):
    def add_one(index, total):
        column = lax.dynamic_index_in_dim(codes, index, 1, keepdims=False)
        table = lax.dynamic_index_in_dim(tables, index, 1, keepdims=False).astype(jnp.float32)
        return total + jnp.take(table, column, axis=1)

    distance = lax.fori_loop(0, M, add_one, jnp.zeros((Q, DB_ROWS), jnp.float32))
    matched = (distance <= limits[:, None].astype(jnp.float32)).astype(jnp.int32)
    hit_count = jnp.sum(matched, axis=1).astype(jnp.int32)
    running = jnp.cumsum(matched, axis=1).astype(jnp.int32)
    slot_index = jnp.arange(SLOTS, dtype=jnp.int32)

    def locate(row):
        return jnp.searchsorted(row, slot_index, side="right").astype(jnp.int32)

    found = jax.vmap(locate)(running)
    hit_ids = jnp.where(slot_index[None, :] < hit_count[:, None], found, -1).astype(jnp.int32)
    return hit_ids, hit_count
```

```python
import functools

import jax
import jax.numpy as jnp
from jax import lax
from jax.experimental import pallas as pl
from jax.experimental.pallas import tpu as pltpu
from jax.sharding import PartitionSpec as P

K = 256
SLOTS = 128
LANES = 128
F8 = jnp.float8_e4m3fn
COLS = 256
MESH = pl.DeviceIdType.MESH


def flip(index, other, size):
    both = 0
    bit = 1
    while bit < size:
        both = both + bit * (((index // bit) % 2) * ((other // bit) % 2))
        bit *= 2
    return index + other - 2 * both


def kernel(
    groups,
    parts,
    codes_hbm,
    tables_hbm,
    limits_hbm,
    ids_ref,
    count_ref,
    codes_raw,
    tables_raw,
    limits_raw,
    codes_all,
    tables_ref,
    part,
    recv1,
    send2,
    recv2,
    running,
    total,
    chosen,
    load_sem,
    code_send,
    code_recv,
    send1_sem,
    recv1_sem,
    send2_sem,
    recv2_sem,
):
    db = lax.axis_index("db")
    sub = lax.axis_index("sub")
    low = sub % 2
    high = sub // 2
    near = sub + 1 - 2 * low
    far = sub + 2 - 4 * high
    width, rows = codes_raw.shape
    mine = ids_ref.shape[0]
    half = groups // 2
    partner = flip(db, 1, groups)

    barrier = pltpu.get_barrier_semaphore()
    pl.semaphore_signal(barrier, inc=1, device_id={"sub": far}, device_id_type=MESH)
    for step in range(1, half):
        pl.semaphore_signal(
            barrier, inc=1, device_id={"db": flip(db, 2 * step, groups)}, device_id_type=MESH
        )
    pl.semaphore_signal(barrier, inc=1, device_id={"db": partner}, device_id_type=MESH)
    pl.semaphore_signal(barrier, inc=1, device_id={"sub": near}, device_id_type=MESH)

    load_codes = pltpu.make_async_copy(codes_hbm, codes_raw, load_sem.at[0])
    load_tables = pltpu.make_async_copy(tables_hbm, tables_raw, load_sem.at[1])
    load_limits = pltpu.make_async_copy(limits_hbm, limits_raw, load_sem.at[2])
    load_codes.start()
    load_tables.start()
    load_limits.start()

    def code_copy(step):
        return pltpu.make_async_remote_copy(
            src_ref=codes_all.at[db],
            dst_ref=codes_all.at[db],
            send_sem=code_send.at[step],
            recv_sem=code_recv.at[step],
            device_id={"db": flip(db, step, groups)},
            device_id_type=MESH,
        )

    def relay_copy(step):
        source = flip(db, step, groups)
        return pltpu.make_async_remote_copy(
            src_ref=codes_all.at[source],
            dst_ref=codes_all.at[source],
            send_sem=code_send.at[step + 1],
            recv_sem=code_recv.at[step + 1],
            device_id={"db": partner},
            device_id_type=MESH,
        )

    def near_copy(source):
        return pltpu.make_async_remote_copy(
            src_ref=part.at[source, :, 1 - low],
            dst_ref=recv1.at[source],
            send_sem=send1_sem.at[source],
            recv_sem=recv1_sem.at[source],
            device_id={"sub": near},
            device_id_type=MESH,
        )

    def far_copy(source):
        return pltpu.make_async_remote_copy(
            src_ref=send2.at[source],
            dst_ref=recv2.at[source],
            send_sem=send2_sem.at[source],
            recv_sem=recv2_sem.at[source],
            device_id={"sub": far},
            device_id_type=MESH,
        )

    load_codes.wait()
    codes_all[db] = codes_raw[...].astype(jnp.float32).astype(jnp.bfloat16)
    pl.semaphore_wait(barrier, half + 2)
    for step in range(half - 1, 0, -1):
        code_copy(2 * step).start()
    code_copy(1).start()

    load_tables.wait()
    tables_ref[...] = jnp.swapaxes(tables_raw[...], 0, 1)
    load_limits.wait()

    centroid = lax.broadcasted_iota(jnp.int32, (K, LANES), 0).astype(jnp.float32)
    centroid = centroid.astype(jnp.bfloat16).reshape(K // 16, 16, LANES)
    centroid = jnp.concatenate([centroid] * (COLS // LANES), axis=2)

    def order(place):
        return 2 * (place % half) + place // half

    def pass_on(step):
        source = flip(db, step, groups)
        near_copy(source).wait_recv()
        send2[source] = part[source, 1 - high, low] + recv1[source, 1 - high]
        far_copy(source).start()

    def score(place, carry):
        step = order(place)
        source = flip(db, step, groups)

        @pl.when(place > 0)
        def _():
            code_copy(step).wait_recv()

            @pl.when(place < half)
            def _():
                relay_copy(step).start()

        def tile(j, carry):
            start = pl.multiple_of(j * COLS, COLS)
            local = codes_all[source, :, pl.ds(start, COLS)].astype(jnp.float32)
            acc = None
            for m in range(width):
                row = jnp.broadcast_to(local[m : m + 1, :], (16, COLS)).astype(jnp.bfloat16)
                hot = jnp.where((centroid == row[None]).reshape(K, COLS), F8(1), F8(0))
                term = lax.dot_general(
                    tables_ref[m],
                    hot,
                    (((1,), (0,)), ((), ())),
                    preferred_element_type=jnp.float32,
                )
                acc = term if acc is None else acc + term
            part[source, :, :, :, pl.ds(start, COLS)] = acc.reshape(2, 2, mine, COLS)
            return carry

        lax.fori_loop(0, rows // COLS, tile, 0, unroll=True)
        near_copy(source).start()

        @pl.when(place > 0)
        def _():
            pass_on(order(place - 1))

        return carry

    lax.fori_loop(0, groups, score, 0)
    pass_on(groups - 1)

    diagonal = lax.broadcasted_iota(jnp.int32, (mine, mine), 0) == lax.broadcasted_iota(
        jnp.int32, (mine, mine), 1
    )
    queries = limits_raw.shape[1]
    first = (db * parts + sub) * mine
    here = lax.broadcasted_iota(jnp.int32, (mine, queries), 1) == (
        first + lax.broadcasted_iota(jnp.int32, (mine, queries), 0)
    )
    limit_row = jnp.broadcast_to(limits_raw[...].astype(jnp.float32), (mine, queries))
    limit = jnp.sum(jnp.where(here, limit_row, 0.0), axis=1, keepdims=True)
    limit = jnp.broadcast_to(limit, (mine, LANES))
    blocks = rows // LANES
    upper_row = lax.broadcasted_iota(jnp.int32, (LANES, 2 * LANES), 0)
    upper_col = lax.broadcasted_iota(jnp.int32, (LANES, 2 * LANES), 1)
    upper = jnp.where(upper_row <= upper_col, 1.0, 0.0).astype(jnp.bfloat16)

    def match(step, carry):
        source = flip(db, 2 * (step % half) + step // half, groups)
        far_copy(source).wait_recv()
        flags = []
        for b in range(blocks):
            cut = pl.ds(b * LANES, LANES)
            distance = (
                part[source, high, low, :, cut]
                + recv1[source, high, :, cut]
                + recv2[source, :, cut]
            )
            flags.append(jnp.where(distance <= limit, 1.0, 0.0).astype(jnp.bfloat16))
        sums = jnp.dot(
            jnp.concatenate(flags, axis=0), upper, preferred_element_type=jnp.float32
        )
        here = pl.ds(pl.multiple_of(source * (blocks * mine), blocks * mine), blocks * mine)
        running[here, :] = sums[:, :LANES]
        total[here, :] = sums[:, LANES:]
        return carry

    lax.fori_loop(0, groups, match, 0)

    slot = lax.broadcasted_iota(jnp.int32, (mine, SLOTS), 1).astype(jnp.float32)

    def choose(b, carry):
        before, base, index, was = carry
        here = pl.ds(pl.multiple_of(b * mine, mine), mine)
        after = before + total[here, :]
        passed = jnp.where(after <= slot, 1.0, 0.0)
        chosen[here, :] = was - passed
        return after, jnp.where(after <= slot, after, base), index + passed, passed

    zero = jnp.zeros((mine, SLOTS), jnp.float32)
    found, base, index, _ = lax.fori_loop(
        0, groups * blocks, choose, (zero, zero, zero, zero + 1.0), unroll=8
    )
    rest = slot - base

    out = []
    for q in range(mine):
        every = pl.ds(q, groups * blocks, stride=mine)
        picked = lax.dot_general(
            running[every, :].astype(jnp.bfloat16),
            chosen[every, :].astype(jnp.bfloat16),
            (((0,), (0,)), ((), ())),
            preferred_element_type=jnp.float32,
        )
        below = jnp.where(picked <= rest[q : q + 1, :], 1.0, 0.0)
        out.append(jnp.sum(below, axis=0, keepdims=True))
    inside = jnp.concatenate(out, axis=0)
    ids_ref[...] = jnp.where(slot < found, index * LANES + inside, -1.0).astype(jnp.int32)
    count_ref[...] = jnp.sum(
        jnp.where(diagonal, found[:, :mine], 0.0), axis=0, keepdims=True
    ).astype(jnp.int32)

    def drain(step, carry):
        source = flip(db, step, groups)

        @pl.when(step > 0)
        def _():
            code_copy(step).wait_send()

        near_copy(source).wait_send()
        far_copy(source).wait_send()
        return carry

    lax.fori_loop(0, groups, drain, 0)


def per_device(groups, parts, codes, tables, limits):
    assert parts == 4 and groups & (groups - 1) == 0
    rows, width = codes.shape
    queries = tables.shape[0]
    mine = queries // parts
    blocks = groups * rows // LANES
    ids, counts = pl.pallas_call(
        functools.partial(kernel, groups, parts),
        out_shape=(
            jax.ShapeDtypeStruct((mine, SLOTS), jnp.int32),
            jax.ShapeDtypeStruct((1, mine), jnp.int32),
        ),
        in_specs=[pl.BlockSpec(memory_space=pl.ANY)] * 3,
        out_specs=[pl.BlockSpec(memory_space=pltpu.VMEM)] * 2,
        scratch_shapes=[
            pltpu.VMEM((width, rows), jnp.int32),
            pltpu.VMEM(tables.shape, jnp.bfloat16),
            pltpu.VMEM((1, limits.shape[0]), jnp.int32),
            pltpu.VMEM((groups, width, rows), jnp.bfloat16),
            pltpu.VMEM((width, queries, K), jnp.bfloat16),
            pltpu.VMEM((groups, 2, 2, mine, rows), jnp.float32),
            pltpu.VMEM((groups, 2, mine, rows), jnp.float32),
            pltpu.VMEM((groups, mine, rows), jnp.float32),
            pltpu.VMEM((groups, mine, rows), jnp.float32),
            pltpu.VMEM((blocks * mine, LANES), jnp.float32),
            pltpu.VMEM((blocks * mine, LANES), jnp.float32),
            pltpu.VMEM((blocks * mine, LANES), jnp.float32),
            pltpu.SemaphoreType.DMA((3,)),
            pltpu.SemaphoreType.DMA((groups,)),
            pltpu.SemaphoreType.DMA((groups,)),
            pltpu.SemaphoreType.DMA((groups,)),
            pltpu.SemaphoreType.DMA((groups,)),
            pltpu.SemaphoreType.DMA((groups,)),
            pltpu.SemaphoreType.DMA((groups,)),
        ],
        compiler_params=pltpu.CompilerParams(
            collective_id=0, has_side_effects=True, vmem_limit_bytes=60 * 1024 * 1024
        ),
        name="retrieve",
    )(codes.T, tables, limits[None, :])
    return ids, counts[0]


def solution(mesh):
    placed = (P("db", "sub"), P("db", "sub", None), P())
    return jax.shard_map(
        functools.partial(per_device, mesh.shape["db"], mesh.shape["sub"]),
        mesh=mesh,
        in_specs=placed,
        out_specs=(P(("db", "sub"), None), P(("db", "sub"))),
        check_vma=False,
    )
```

```python
import functools

import jax
import jax.numpy as jnp
from jax import lax
from jax.experimental import pallas as pl
from jax.experimental.pallas import tpu as pltpu
from jax.sharding import PartitionSpec as P

K = 256
SLOTS = 128
LANES = 128
F8 = jnp.float8_e4m3fn
UNIT = 2.0**-10
BITS = 22
TOP = 2.0 ** (BITS - 10) - UNIT
PART = BITS - 12
COLS = 256
MESH = pl.DeviceIdType.MESH


def flip(index, other, size):
    both = 0
    bit = 1
    while bit < size:
        both = both + bit * (((index // bit) % 2) * ((other // bit) % 2))
        bit *= 2
    return index + other - 2 * both


def kernel(
    groups,
    parts,
    codes_hbm,
    tables_hbm,
    limits_hbm,
    ids_ref,
    count_ref,
    codes_raw,
    tables_raw,
    limits_raw,
    codes_all,
    tables_ref,
    part,
    recv1,
    send2,
    recv2,
    running,
    total,
    chosen,
    load_sem,
    code_send,
    code_recv,
    send1_sem,
    recv1_sem,
    send2_sem,
    recv2_sem,
):
    db = lax.axis_index("db")
    sub = lax.axis_index("sub")
    low = sub % 2
    high = sub // 2
    near = sub + 1 - 2 * low
    far = sub + 2 - 4 * high
    width, rows = codes_raw.shape
    mine = ids_ref.shape[0]
    quarter = rows // 4
    half = groups // 2
    partner = flip(db, 1, groups)

    barrier = pltpu.get_barrier_semaphore()
    pl.semaphore_signal(barrier, inc=1, device_id={"sub": far}, device_id_type=MESH)
    for step in range(1, half):
        pl.semaphore_signal(
            barrier, inc=1, device_id={"db": flip(db, 2 * step, groups)}, device_id_type=MESH
        )
    pl.semaphore_signal(barrier, inc=1, device_id={"db": partner}, device_id_type=MESH)
    pl.semaphore_signal(barrier, inc=1, device_id={"sub": near}, device_id_type=MESH)

    load_codes = pltpu.make_async_copy(codes_hbm, codes_raw, load_sem.at[0])
    load_tables = pltpu.make_async_copy(tables_hbm, tables_raw, load_sem.at[1])
    load_limits = pltpu.make_async_copy(limits_hbm, limits_raw, load_sem.at[2])
    load_codes.start()
    load_tables.start()
    load_limits.start()

    def code_copy(step):
        return pltpu.make_async_remote_copy(
            src_ref=codes_all.at[db],
            dst_ref=codes_all.at[db],
            send_sem=code_send.at[step],
            recv_sem=code_recv.at[step],
            device_id={"db": flip(db, step, groups)},
            device_id_type=MESH,
        )

    def relay_copy(step):
        source = flip(db, step, groups)
        return pltpu.make_async_remote_copy(
            src_ref=codes_all.at[source],
            dst_ref=codes_all.at[source],
            send_sem=code_send.at[step + 1],
            recv_sem=code_recv.at[step + 1],
            device_id={"db": partner},
            device_id_type=MESH,
        )

    def near_copy(source):
        return pltpu.make_async_remote_copy(
            src_ref=part.at[source, :, 1 - low],
            dst_ref=recv1.at[source],
            send_sem=send1_sem.at[source],
            recv_sem=recv1_sem.at[source],
            device_id={"sub": near},
            device_id_type=MESH,
        )

    def far_copy(source):
        return pltpu.make_async_remote_copy(
            src_ref=send2.at[source],
            dst_ref=recv2.at[source],
            send_sem=send2_sem.at[source],
            recv_sem=recv2_sem.at[source],
            device_id={"sub": far},
            device_id_type=MESH,
        )

    load_codes.wait()
    codes_all[db] = codes_raw[...].astype(jnp.float32).astype(jnp.bfloat16)
    pl.semaphore_wait(barrier, half + 2)
    for step in range(half - 1, 0, -1):
        code_copy(2 * step).start()
    code_copy(1).start()

    load_tables.wait()
    tables_ref[...] = jnp.swapaxes(tables_raw[...], 0, 1)
    load_limits.wait()

    centroid = lax.broadcasted_iota(jnp.int32, (K, LANES), 0).astype(jnp.float32)
    centroid = centroid.astype(jnp.bfloat16).reshape(K // 16, 16, LANES)
    centroid = jnp.concatenate([centroid] * (COLS // LANES), axis=2)

    def order(place):
        return 2 * (place % half) + place // half

    def pass_on(step):
        source = flip(db, step, groups)
        near_copy(source).wait_recv()
        value = part[source, 1 - high, low] + recv1[source, 1 - high]
        count = (jnp.minimum(value, TOP) * (1.0 / UNIT)).astype(jnp.int32)
        last = count[:, 3 * quarter :]
        for k in range(3):
            piece = jnp.bitwise_and(lax.shift_right_logical(last, k * PART), (1 << PART) - 1)
            send2[source, k] = jnp.bitwise_or(
                count[:, k * quarter : (k + 1) * quarter], lax.shift_left(piece, BITS)
            )
        far_copy(source).start()

    def score(place, carry):
        step = order(place)
        source = flip(db, step, groups)

        @pl.when(place == 1)
        def _():
            pass_on(order(place - 1))

        @pl.when(place > 0)
        def _():
            code_copy(step).wait_recv()

            @pl.when(place < half)
            def _():
                relay_copy(step).start()

        def tile(j, carry):
            start = pl.multiple_of(j * COLS, COLS)
            local = codes_all[source, :, pl.ds(start, COLS)].astype(jnp.float32)
            acc = None
            for m in range(width):
                row = jnp.broadcast_to(local[m : m + 1, :], (16, COLS)).astype(jnp.bfloat16)
                hot = jnp.where((centroid == row[None]).reshape(K, COLS), F8(1), F8(0))
                term = lax.dot_general(
                    tables_ref[m],
                    hot,
                    (((1,), (0,)), ((), ())),
                    preferred_element_type=jnp.float32,
                )
                acc = term if acc is None else acc + term
            part[source, :, :, :, pl.ds(start, COLS)] = acc.reshape(2, 2, mine, COLS)
            return carry

        tiles = rows // COLS
        lax.fori_loop(0, tiles // 2, tile, 0, unroll=True)

        @pl.when(place > 2)
        def _():
            pass_on(order(place - 2))

        lax.fori_loop(tiles // 2, tiles, tile, 0, unroll=True)
        near_copy(source).start()
        return carry

    lax.fori_loop(0, groups, score, 0)
    pass_on(order(groups - 2))
    pass_on(order(groups - 1))

    diagonal = lax.broadcasted_iota(jnp.int32, (mine, mine), 0) == lax.broadcasted_iota(
        jnp.int32, (mine, mine), 1
    )
    queries = limits_raw.shape[1]
    first = (db * parts + sub) * mine
    here = lax.broadcasted_iota(jnp.int32, (mine, queries), 1) == (
        first + lax.broadcasted_iota(jnp.int32, (mine, queries), 0)
    )
    limit_row = jnp.broadcast_to(limits_raw[...].astype(jnp.float32), (mine, queries))
    limit = jnp.sum(jnp.where(here, limit_row, 0.0), axis=1, keepdims=True)
    limit = jnp.broadcast_to(limit, (mine, LANES))
    blocks = rows // LANES
    upper_row = lax.broadcasted_iota(jnp.int32, (LANES, 2 * LANES), 0)
    upper_col = lax.broadcasted_iota(jnp.int32, (LANES, 2 * LANES), 1)
    upper = jnp.where(upper_row <= upper_col, 1.0, 0.0).astype(jnp.bfloat16)

    def match(step, carry):
        source = flip(db, 2 * (step % half) + step // half, groups)
        far_copy(source).wait_recv()
        words = [recv2[source, k] for k in range(3)]
        sent = [jnp.bitwise_and(word, (1 << BITS) - 1) for word in words]
        rest = [lax.shift_right_logical(word, BITS) for word in words]
        for k in range(1, 3):
            rest[0] = jnp.bitwise_or(rest[0], lax.shift_left(rest[k], k * PART))
        sent.append(rest[0])
        flags = []
        for b in range(blocks):
            cut = pl.ds(b * LANES, LANES)
            at = b * LANES % quarter
            other = sent[b * LANES // quarter][:, at : at + LANES].astype(jnp.float32)
            distance = (
                part[source, high, low, :, cut] + recv1[source, high, :, cut] + other * UNIT
            )
            flags.append(jnp.where(distance <= limit, 1.0, 0.0).astype(jnp.bfloat16))
        sums = jnp.dot(
            jnp.concatenate(flags, axis=0), upper, preferred_element_type=jnp.float32
        )
        here = pl.ds(pl.multiple_of(source * (blocks * mine), blocks * mine), blocks * mine)
        running[here, :] = sums[:, :LANES]
        total[here, :] = sums[:, LANES:]
        return carry

    lax.fori_loop(0, groups, match, 0)

    slot = lax.broadcasted_iota(jnp.int32, (mine, SLOTS), 1).astype(jnp.float32)

    def choose(b, carry):
        before, base, index, was = carry
        here = pl.ds(pl.multiple_of(b * mine, mine), mine)
        after = before + total[here, :]
        passed = jnp.where(after <= slot, 1.0, 0.0)
        chosen[here, :] = was - passed
        return after, jnp.where(after <= slot, after, base), index + passed, passed

    zero = jnp.zeros((mine, SLOTS), jnp.float32)
    found, base, index, _ = lax.fori_loop(
        0, groups * blocks, choose, (zero, zero, zero, zero + 1.0), unroll=8
    )
    rest = slot - base

    out = []
    for q in range(mine):
        every = pl.ds(q, groups * blocks, stride=mine)
        picked = lax.dot_general(
            running[every, :].astype(jnp.bfloat16),
            chosen[every, :].astype(jnp.bfloat16),
            (((0,), (0,)), ((), ())),
            preferred_element_type=jnp.float32,
        )
        below = jnp.where(picked <= rest[q : q + 1, :], 1.0, 0.0)
        out.append(jnp.sum(below, axis=0, keepdims=True))
    inside = jnp.concatenate(out, axis=0)
    ids_ref[...] = jnp.where(slot < found, index * LANES + inside, -1.0).astype(jnp.int32)
    count_ref[...] = jnp.sum(
        jnp.where(diagonal, found[:, :mine], 0.0), axis=0, keepdims=True
    ).astype(jnp.int32)

    def drain(step, carry):
        source = flip(db, step, groups)

        @pl.when(step > 0)
        def _():
            code_copy(step).wait_send()

        near_copy(source).wait_send()
        far_copy(source).wait_send()
        return carry

    lax.fori_loop(0, groups, drain, 0)


def emit(ids_in, count_in, ids_ref, count_ref, sem):
    ids = pltpu.make_async_copy(ids_in, ids_ref, sem.at[0])
    count = pltpu.make_async_copy(count_in, count_ref, sem.at[1])
    ids.start()
    count.start()
    ids.wait()
    count.wait()


def per_device(groups, parts, codes, tables, limits):
    assert parts == 4 and groups & (groups - 1) == 0
    rows, width = codes.shape
    queries = tables.shape[0]
    mine = queries // parts
    blocks = groups * rows // LANES
    assert 2 * width * 128 <= 2 ** (BITS - 10)
    held = [
        pltpu.with_memory_space_constraint(array, pltpu.HBM)
        for array in (codes.T, tables, limits[None, :])
    ]
    ids, counts = pl.pallas_call(
        functools.partial(kernel, groups, parts),
        out_shape=(
            jax.ShapeDtypeStruct((mine, SLOTS), jnp.int32),
            jax.ShapeDtypeStruct((1, mine), jnp.int32),
        ),
        in_specs=[pl.BlockSpec(memory_space=pl.ANY)] * 3,
        out_specs=[pl.BlockSpec(memory_space=pltpu.VMEM)] * 2,
        scratch_shapes=[
            pltpu.VMEM((width, rows), jnp.int32),
            pltpu.VMEM(tables.shape, jnp.bfloat16),
            pltpu.VMEM((1, limits.shape[0]), jnp.int32),
            pltpu.VMEM((groups, width, rows), jnp.bfloat16),
            pltpu.VMEM((width, queries, K), jnp.bfloat16),
            pltpu.VMEM((groups, 2, 2, mine, rows), jnp.float32),
            pltpu.VMEM((groups, 2, mine, rows), jnp.float32),
            pltpu.VMEM((groups, 3, mine, rows // 4), jnp.int32),
            pltpu.VMEM((groups, 3, mine, rows // 4), jnp.int32),
            pltpu.VMEM((blocks * mine, LANES), jnp.float32),
            pltpu.VMEM((blocks * mine, LANES), jnp.float32),
            pltpu.VMEM((blocks * mine, LANES), jnp.float32),
            pltpu.SemaphoreType.DMA((3,)),
            pltpu.SemaphoreType.DMA((groups,)),
            pltpu.SemaphoreType.DMA((groups,)),
            pltpu.SemaphoreType.DMA((groups,)),
            pltpu.SemaphoreType.DMA((groups,)),
            pltpu.SemaphoreType.DMA((groups,)),
            pltpu.SemaphoreType.DMA((groups,)),
        ],
        compiler_params=pltpu.CompilerParams(
            collective_id=0, has_side_effects=True, vmem_limit_bytes=48 * 1024 * 1024
        ),
        name="retrieve",
    )(*held)

    ids, counts = pl.pallas_call(
        emit,
        out_shape=(
            jax.ShapeDtypeStruct((mine, SLOTS), jnp.int32),
            jax.ShapeDtypeStruct((1, mine), jnp.int32),
        ),
        in_specs=[pl.BlockSpec(memory_space=pl.ANY)] * 2,
        out_specs=[pl.BlockSpec(memory_space=pltpu.HBM)] * 2,
        scratch_shapes=[pltpu.SemaphoreType.DMA((2,))],
        compiler_params=pltpu.CompilerParams(vmem_limit_bytes=1024 * 1024),
        name="emit",
    )(ids, counts)
    return ids, counts[0]


def solution(mesh):
    placed = (P("db", "sub"), P("db", "sub", None), P())
    return jax.shard_map(
        functools.partial(per_device, mesh.shape["db"], mesh.shape["sub"]),
        mesh=mesh,
        in_specs=placed,
        out_specs=(P(("db", "sub"), None), P(("db", "sub"))),
        check_vma=False,
    )
```

```python
import functools

import jax
import jax.numpy as jnp
from jax import lax
from jax.experimental import pallas as pl
from jax.experimental.pallas import tpu as pltpu
from jax.sharding import PartitionSpec as P

K = 256
SLOTS = 128
LANES = 128
F8 = jnp.float8_e4m3fn
UNIT = 2.0**-10
BITS = 22
TOP = 2.0 ** (BITS - 10) - UNIT
PART = BITS - 12
COLS = 256
BATCH = 2
MESH = pl.DeviceIdType.MESH


def flip(index, other, size):
    both = 0
    bit = 1
    while bit < size:
        both = both + bit * (((index // bit) % 2) * ((other // bit) % 2))
        bit *= 2
    return index + other - 2 * both


def kernel(
    groups,
    parts,
    codes_hbm,
    tables_hbm,
    limits_hbm,
    ids_ref,
    count_ref,
    codes_raw,
    tables_raw,
    limits_raw,
    codes_all,
    tables_ref,
    part,
    recv1,
    send2,
    recv2,
    running,
    total,
    chosen,
    load_sem,
    code_send,
    code_recv,
    send1_sem,
    recv1_sem,
    send2_sem,
    recv2_sem,
):
    db = lax.axis_index("db")
    sub = lax.axis_index("sub")
    low = sub % 2
    high = sub // 2
    near = sub + 1 - 2 * low
    far = sub + 2 - 4 * high
    width, rows = codes_raw.shape
    mine = ids_ref.shape[0]
    quarter = rows // 4
    half = groups // 2
    partner = flip(db, 1, groups)

    barrier = pltpu.get_barrier_semaphore()
    pl.semaphore_signal(barrier, inc=1, device_id={"sub": far}, device_id_type=MESH)
    for step in range(1, half):
        pl.semaphore_signal(
            barrier, inc=1, device_id={"db": flip(db, 2 * step, groups)}, device_id_type=MESH
        )
    pl.semaphore_signal(barrier, inc=1, device_id={"db": partner}, device_id_type=MESH)
    pl.semaphore_signal(barrier, inc=1, device_id={"sub": near}, device_id_type=MESH)

    load_codes = pltpu.make_async_copy(codes_hbm, codes_raw, load_sem.at[0])
    load_tables = pltpu.make_async_copy(tables_hbm, tables_raw, load_sem.at[1])
    load_limits = pltpu.make_async_copy(limits_hbm, limits_raw, load_sem.at[2])
    load_codes.start()
    load_tables.start()
    load_limits.start()

    def code_copy(step):
        return pltpu.make_async_remote_copy(
            src_ref=codes_all.at[db],
            dst_ref=codes_all.at[db],
            send_sem=code_send.at[step],
            recv_sem=code_recv.at[step],
            device_id={"db": flip(db, step, groups)},
            device_id_type=MESH,
        )

    def relay_copy(step):
        source = flip(db, step, groups)
        return pltpu.make_async_remote_copy(
            src_ref=codes_all.at[source],
            dst_ref=codes_all.at[source],
            send_sem=code_send.at[step + 1],
            recv_sem=code_recv.at[step + 1],
            device_id={"db": partner},
            device_id_type=MESH,
        )

    def near_copy(source):
        return pltpu.make_async_remote_copy(
            src_ref=part.at[source, :, 1 - low],
            dst_ref=recv1.at[source],
            send_sem=send1_sem.at[source],
            recv_sem=recv1_sem.at[source],
            device_id={"sub": near},
            device_id_type=MESH,
        )

    def far_copy(source):
        return pltpu.make_async_remote_copy(
            src_ref=send2.at[source],
            dst_ref=recv2.at[source],
            send_sem=send2_sem.at[source],
            recv_sem=recv2_sem.at[source],
            device_id={"sub": far},
            device_id_type=MESH,
        )

    load_codes.wait()
    codes_all[db] = codes_raw[...].astype(jnp.float32).astype(jnp.bfloat16)
    pl.semaphore_wait(barrier, half + 2)
    for step in range(half - 1, 0, -1):
        code_copy(2 * step).start()
    code_copy(1).start()

    load_tables.wait()
    tables_ref[...] = jnp.swapaxes(tables_raw[...], 0, 1)
    load_limits.wait()

    centroid = lax.broadcasted_iota(jnp.int32, (K, LANES), 0).astype(jnp.float32)
    centroid = centroid.astype(jnp.bfloat16).reshape(K // 16, 16, LANES)
    centroid = jnp.concatenate([centroid] * (COLS // LANES), axis=2)

    def order(place):
        return 2 * (place % half) + place // half

    def pass_on(step):
        source = flip(db, step, groups)
        near_copy(source).wait_recv()
        value = part[source, 1 - high, low] + recv1[source, 1 - high]
        count = (jnp.minimum(value, TOP) * (1.0 / UNIT)).astype(jnp.int32)
        last = count[:, 3 * quarter :]
        for k in range(3):
            piece = jnp.bitwise_and(lax.shift_right_logical(last, k * PART), (1 << PART) - 1)
            send2[source, k] = jnp.bitwise_or(
                count[:, k * quarter : (k + 1) * quarter], lax.shift_left(piece, BITS)
            )
        far_copy(source).start()

    def score(place, carry):
        step = order(place)
        source = flip(db, step, groups)

        @pl.when(place == 1)
        def _():
            pass_on(order(place - 1))

        @pl.when(place > 0)
        def _():
            code_copy(step).wait_recv()

            @pl.when(place < half)
            def _():
                relay_copy(step).start()

        def tile(j, carry):
            start = pl.multiple_of(j * COLS, COLS)
            local = codes_all[source, :, pl.ds(start, COLS)].astype(jnp.float32)
            acc = None
            for m in range(width):
                row = jnp.broadcast_to(local[m : m + 1, :], (16, COLS)).astype(jnp.bfloat16)
                hot = jnp.where((centroid == row[None]).reshape(K, COLS), F8(1), F8(0))
                term = lax.dot_general(
                    tables_ref[m],
                    hot,
                    (((1,), (0,)), ((), ())),
                    preferred_element_type=jnp.float32,
                )
                acc = term if acc is None else acc + term
            part[source, :, :, :, pl.ds(start, COLS)] = acc.reshape(2, 2, mine, COLS)
            return carry

        lax.fori_loop(0, rows // COLS, tile, 0, unroll=True)
        near_copy(source).start()

        @pl.when(place > 1)
        def _():
            pass_on(order(place - 1))

        return carry

    lax.fori_loop(0, groups, score, 0)
    pass_on(order(groups - 1))

    diagonal = lax.broadcasted_iota(jnp.int32, (mine, mine), 0) == lax.broadcasted_iota(
        jnp.int32, (mine, mine), 1
    )
    queries = limits_raw.shape[1]
    first = (db * parts + sub) * mine
    here = lax.broadcasted_iota(jnp.int32, (mine, queries), 1) == (
        first + lax.broadcasted_iota(jnp.int32, (mine, queries), 0)
    )
    limit_row = jnp.broadcast_to(limits_raw[...].astype(jnp.float32), (mine, queries))
    limit = jnp.sum(jnp.where(here, limit_row, 0.0), axis=1, keepdims=True)
    limit = jnp.broadcast_to(limit, (mine, LANES))
    blocks = rows // LANES
    upper_row = lax.broadcasted_iota(jnp.int32, (LANES, 2 * LANES), 0)
    upper_col = lax.broadcasted_iota(jnp.int32, (LANES, 2 * LANES), 1)
    upper = jnp.where(upper_row <= upper_col, 1.0, 0.0).astype(jnp.bfloat16)

    def match(turn, carry):
        flags = []
        for k in range(BATCH):
            source = flip(db, order(turn * BATCH + k), groups)
            far_copy(source).wait_recv()
            words = [recv2[source, k] for k in range(3)]
            sent = [jnp.bitwise_and(word, (1 << BITS) - 1) for word in words]
            rest = [lax.shift_right_logical(word, BITS) for word in words]
            for k in range(1, 3):
                rest[0] = jnp.bitwise_or(rest[0], lax.shift_left(rest[k], k * PART))
            sent.append(rest[0])
            for b in range(blocks):
                cut = pl.ds(b * LANES, LANES)
                at = b * LANES % quarter
                other = sent[b * LANES // quarter][:, at : at + LANES].astype(jnp.float32)
                distance = (
                    part[source, high, low, :, cut] + recv1[source, high, :, cut] + other * UNIT
                )
                flags.append(jnp.where(distance <= limit, 1.0, 0.0).astype(jnp.bfloat16))
        sums = jnp.dot(
            jnp.concatenate(flags, axis=0), upper, preferred_element_type=jnp.float32
        )
        size = blocks * mine
        for k in range(BATCH):
            source = flip(db, order(turn * BATCH + k), groups)
            here = pl.ds(pl.multiple_of(source * size, size), size)
            running[here, :] = sums[k * size : (k + 1) * size, :LANES]
            total[here, :] = sums[k * size : (k + 1) * size, LANES:]
        return carry

    lax.fori_loop(0, groups // BATCH, match, 0)

    slot = lax.broadcasted_iota(jnp.int32, (mine, SLOTS), 1).astype(jnp.float32)

    def choose(b, carry):
        before, base, index, was = carry
        here = pl.ds(pl.multiple_of(b * mine, mine), mine)
        after = before + total[here, :]
        passed = jnp.where(after <= slot, 1.0, 0.0)
        chosen[here, :] = was - passed
        return after, jnp.where(after <= slot, after, base), index + passed, passed

    zero = jnp.zeros((mine, SLOTS), jnp.float32)
    found, base, index, _ = lax.fori_loop(
        0, groups * blocks, choose, (zero, zero, zero, zero + 1.0), unroll=8
    )
    rest = slot - base

    out = []
    for q in range(mine):
        every = pl.ds(q, groups * blocks, stride=mine)
        picked = lax.dot_general(
            running[every, :].astype(jnp.bfloat16),
            chosen[every, :].astype(jnp.bfloat16),
            (((0,), (0,)), ((), ())),
            preferred_element_type=jnp.float32,
        )
        below = jnp.where(picked <= rest[q : q + 1, :], 1.0, 0.0)
        out.append(jnp.sum(below, axis=0, keepdims=True))
    inside = jnp.concatenate(out, axis=0)
    ids_ref[...] = jnp.where(slot < found, index * LANES + inside, -1.0).astype(jnp.int32)
    count_ref[...] = jnp.sum(
        jnp.where(diagonal, found[:, :mine], 0.0), axis=0, keepdims=True
    ).astype(jnp.int32)

    def drain(step, carry):
        source = flip(db, step, groups)

        @pl.when(step > 0)
        def _():
            code_copy(step).wait_send()

        near_copy(source).wait_send()
        far_copy(source).wait_send()
        return carry

    lax.fori_loop(0, groups, drain, 0)


def emit(ids_in, count_in, ids_ref, count_ref, sem):
    ids = pltpu.make_async_copy(ids_in, ids_ref, sem.at[0])
    count = pltpu.make_async_copy(count_in, count_ref, sem.at[1])
    ids.start()
    count.start()
    ids.wait()
    count.wait()


def per_device(groups, parts, codes, tables, limits):
    assert parts == 4 and groups & (groups - 1) == 0
    rows, width = codes.shape
    queries = tables.shape[0]
    mine = queries // parts
    blocks = groups * rows // LANES
    assert 2 * width * 128 <= 2 ** (BITS - 10)
    held = [
        pltpu.with_memory_space_constraint(array, pltpu.HBM)
        for array in (codes.T, tables, limits[None, :])
    ]
    ids, counts = pl.pallas_call(
        functools.partial(kernel, groups, parts),
        out_shape=(
            jax.ShapeDtypeStruct((mine, SLOTS), jnp.int32),
            jax.ShapeDtypeStruct((1, mine), jnp.int32),
        ),
        in_specs=[pl.BlockSpec(memory_space=pl.ANY)] * 3,
        out_specs=[pl.BlockSpec(memory_space=pltpu.VMEM)] * 2,
        scratch_shapes=[
            pltpu.VMEM((width, rows), jnp.int32),
            pltpu.VMEM(tables.shape, jnp.bfloat16),
            pltpu.VMEM((1, limits.shape[0]), jnp.int32),
            pltpu.VMEM((groups, width, rows), jnp.bfloat16),
            pltpu.VMEM((width, queries, K), jnp.bfloat16),
            pltpu.VMEM((groups, 2, 2, mine, rows), jnp.float32),
            pltpu.VMEM((groups, 2, mine, rows), jnp.float32),
            pltpu.VMEM((groups, 3, mine, rows // 4), jnp.int32),
            pltpu.VMEM((groups, 3, mine, rows // 4), jnp.int32),
            pltpu.VMEM((blocks * mine, LANES), jnp.float32),
            pltpu.VMEM((blocks * mine, LANES), jnp.float32),
            pltpu.VMEM((blocks * mine, LANES), jnp.float32),
            pltpu.SemaphoreType.DMA((3,)),
            pltpu.SemaphoreType.DMA((groups,)),
            pltpu.SemaphoreType.DMA((groups,)),
            pltpu.SemaphoreType.DMA((groups,)),
            pltpu.SemaphoreType.DMA((groups,)),
            pltpu.SemaphoreType.DMA((groups,)),
            pltpu.SemaphoreType.DMA((groups,)),
        ],
        compiler_params=pltpu.CompilerParams(
            collective_id=0, has_side_effects=True, vmem_limit_bytes=48 * 1024 * 1024
        ),
        name="retrieve",
    )(*held)

    ids, counts = pl.pallas_call(
        emit,
        out_shape=(
            jax.ShapeDtypeStruct((mine, SLOTS), jnp.int32),
            jax.ShapeDtypeStruct((1, mine), jnp.int32),
        ),
        in_specs=[pl.BlockSpec(memory_space=pl.ANY)] * 2,
        out_specs=[pl.BlockSpec(memory_space=pltpu.HBM)] * 2,
        scratch_shapes=[pltpu.SemaphoreType.DMA((2,))],
        compiler_params=pltpu.CompilerParams(vmem_limit_bytes=1024 * 1024),
        name="emit",
    )(ids, counts)
    return ids, counts[0]


def solution(mesh):
    placed = (P("db", "sub"), P("db", "sub", None), P())
    return jax.shard_map(
        functools.partial(per_device, mesh.shape["db"], mesh.shape["sub"]),
        mesh=mesh,
        in_specs=placed,
        out_specs=(P(("db", "sub"), None), P(("db", "sub"))),
        check_vma=False,
    )
```

```python
import functools

import jax
import jax.numpy as jnp
from jax import lax
from jax.experimental import pallas as pl
from jax.experimental.pallas import tpu as pltpu
from jax.sharding import PartitionSpec as P

K = 256
SLOTS = 128
LANES = 128
F8 = jnp.float8_e4m3fn
UNIT = 2.0**-10
BITS = 22
TOP = 2.0 ** (BITS - 10) - UNIT
PART = BITS - 12
COLS = 256
BATCH = 2
MESH = pl.DeviceIdType.MESH


def flip(index, other, size):
    both = 0
    bit = 1
    while bit < size:
        both = both + bit * (((index // bit) % 2) * ((other // bit) % 2))
        bit *= 2
    return index + other - 2 * both


def kernel(
    groups,
    parts,
    codes_hbm,
    tables_hbm,
    limits_hbm,
    ids_ref,
    count_ref,
    codes_raw,
    tables_raw,
    limits_raw,
    codes_all,
    tables_ref,
    part,
    recv1,
    send2,
    recv2,
    running,
    total,
    chosen,
    load_sem,
    code_send,
    code_recv,
    send1_sem,
    recv1_sem,
    send2_sem,
    recv2_sem,
):
    db = lax.axis_index("db")
    sub = lax.axis_index("sub")
    low = sub % 2
    high = sub // 2
    near = sub + 1 - 2 * low
    far = sub + 2 - 4 * high
    width, rows = codes_raw.shape
    mine = ids_ref.shape[0]
    quarter = rows // 4
    half = groups // 2
    partner = flip(db, 1, groups)

    barrier = pltpu.get_barrier_semaphore()
    pl.semaphore_signal(barrier, inc=1, device_id={"sub": far}, device_id_type=MESH)
    for step in range(1, half):
        pl.semaphore_signal(
            barrier, inc=1, device_id={"db": flip(db, 2 * step, groups)}, device_id_type=MESH
        )
    pl.semaphore_signal(barrier, inc=1, device_id={"db": partner}, device_id_type=MESH)
    pl.semaphore_signal(barrier, inc=1, device_id={"sub": near}, device_id_type=MESH)

    load_codes = pltpu.make_async_copy(codes_hbm, codes_raw, load_sem.at[0])
    load_tables = pltpu.make_async_copy(tables_hbm, tables_raw, load_sem.at[1])
    load_limits = pltpu.make_async_copy(limits_hbm, limits_raw, load_sem.at[2])
    load_codes.start()
    load_tables.start()
    load_limits.start()

    def code_copy(step):
        return pltpu.make_async_remote_copy(
            src_ref=codes_all.at[db],
            dst_ref=codes_all.at[db],
            send_sem=code_send.at[step],
            recv_sem=code_recv.at[step],
            device_id={"db": flip(db, step, groups)},
            device_id_type=MESH,
        )

    def relay_copy(step):
        source = flip(db, step, groups)
        return pltpu.make_async_remote_copy(
            src_ref=codes_all.at[source],
            dst_ref=codes_all.at[source],
            send_sem=code_send.at[step + 1],
            recv_sem=code_recv.at[step + 1],
            device_id={"db": partner},
            device_id_type=MESH,
        )

    def near_copy(source):
        return pltpu.make_async_remote_copy(
            src_ref=part.at[source, :, 1 - low],
            dst_ref=recv1.at[source],
            send_sem=send1_sem.at[source],
            recv_sem=recv1_sem.at[source],
            device_id={"sub": near},
            device_id_type=MESH,
        )

    def far_copy(source):
        return pltpu.make_async_remote_copy(
            src_ref=send2.at[source],
            dst_ref=recv2.at[source],
            send_sem=send2_sem.at[source],
            recv_sem=recv2_sem.at[source],
            device_id={"sub": far},
            device_id_type=MESH,
        )

    load_codes.wait()
    codes_all[db] = codes_raw[...].astype(jnp.float32).astype(jnp.bfloat16)
    pl.semaphore_wait(barrier, half + 2)
    code_copy(1).start()
    for step in range(1, half):
        code_copy(2 * step).start()

    load_tables.wait()
    tables_ref[...] = jnp.swapaxes(tables_raw[...], 0, 1)
    load_limits.wait()

    centroid = lax.broadcasted_iota(jnp.int32, (K, LANES), 0).astype(jnp.float32)
    centroid = centroid.astype(jnp.bfloat16).reshape(K // 16, 16, LANES)
    centroid = jnp.concatenate([centroid] * (COLS // LANES), axis=2)

    def order(place):
        return 2 * (place % half) + place // half

    def pass_on(step):
        source = flip(db, step, groups)
        near_copy(source).wait_recv()
        value = part[source, 1 - high, low] + recv1[source, 1 - high]
        count = (jnp.minimum(value, TOP) * (1.0 / UNIT)).astype(jnp.int32)
        last = count[:, 3 * quarter :]
        for k in range(3):
            piece = jnp.bitwise_and(lax.shift_right_logical(last, k * PART), (1 << PART) - 1)
            send2[source, k] = jnp.bitwise_or(
                count[:, k * quarter : (k + 1) * quarter], lax.shift_left(piece, BITS)
            )
        far_copy(source).start()

    def score(place, carry):
        step = order(place)
        source = flip(db, step, groups)

        @pl.when(place == 1)
        def _():
            pass_on(order(place - 1))

        @pl.when(place > 0)
        def _():
            code_copy(step).wait_recv()

            @pl.when(place < half)
            def _():
                relay_copy(step).start()

        def tile(j, carry):
            start = pl.multiple_of(j * COLS, COLS)
            local = codes_all[source, :, pl.ds(start, COLS)].astype(jnp.float32)
            acc = None
            for m in range(width):
                row = jnp.broadcast_to(local[m : m + 1, :], (16, COLS)).astype(jnp.bfloat16)
                hot = jnp.where((centroid == row[None]).reshape(K, COLS), F8(1), F8(0))
                term = lax.dot_general(
                    tables_ref[m],
                    hot,
                    (((1,), (0,)), ((), ())),
                    preferred_element_type=jnp.float32,
                )
                acc = term if acc is None else acc + term
            part[source, :, :, :, pl.ds(start, COLS)] = acc.reshape(2, 2, mine, COLS)
            return carry

        lax.fori_loop(0, rows // COLS, tile, 0, unroll=True)
        near_copy(source).start()

        @pl.when(place > 1)
        def _():
            pass_on(order(place - 1))

        return carry

    lax.fori_loop(0, groups, score, 0)
    pass_on(order(groups - 1))

    diagonal = lax.broadcasted_iota(jnp.int32, (mine, mine), 0) == lax.broadcasted_iota(
        jnp.int32, (mine, mine), 1
    )
    queries = limits_raw.shape[1]
    first = (db * parts + sub) * mine
    here = lax.broadcasted_iota(jnp.int32, (mine, queries), 1) == (
        first + lax.broadcasted_iota(jnp.int32, (mine, queries), 0)
    )
    limit_row = jnp.broadcast_to(limits_raw[...].astype(jnp.float32), (mine, queries))
    limit = jnp.sum(jnp.where(here, limit_row, 0.0), axis=1, keepdims=True)
    limit = jnp.broadcast_to(limit, (mine, LANES))
    blocks = rows // LANES
    upper_row = lax.broadcasted_iota(jnp.int32, (LANES, 2 * LANES), 0)
    upper_col = lax.broadcasted_iota(jnp.int32, (LANES, 2 * LANES), 1)
    upper = jnp.where(upper_row <= upper_col, 1.0, 0.0).astype(jnp.bfloat16)

    def match(turn, carry):
        flags = []
        for k in range(BATCH):
            source = flip(db, order(turn * BATCH + k), groups)
            far_copy(source).wait_recv()
            words = [recv2[source, k] for k in range(3)]
            sent = [jnp.bitwise_and(word, (1 << BITS) - 1) for word in words]
            rest = [lax.shift_right_logical(word, BITS) for word in words]
            for k in range(1, 3):
                rest[0] = jnp.bitwise_or(rest[0], lax.shift_left(rest[k], k * PART))
            sent.append(rest[0])
            for b in range(blocks):
                cut = pl.ds(b * LANES, LANES)
                at = b * LANES % quarter
                other = sent[b * LANES // quarter][:, at : at + LANES].astype(jnp.float32)
                distance = (
                    part[source, high, low, :, cut] + recv1[source, high, :, cut] + other * UNIT
                )
                flags.append(jnp.where(distance <= limit, 1.0, 0.0).astype(jnp.bfloat16))
        sums = jnp.dot(
            jnp.concatenate(flags, axis=0), upper, preferred_element_type=jnp.float32
        )
        size = blocks * mine
        for k in range(BATCH):
            source = flip(db, order(turn * BATCH + k), groups)
            here = pl.ds(pl.multiple_of(source * size, size), size)
            running[here, :] = sums[k * size : (k + 1) * size, :LANES]
            total[here, :] = sums[k * size : (k + 1) * size, LANES:]
        return carry

    lax.fori_loop(0, groups // BATCH, match, 0)

    slot = lax.broadcasted_iota(jnp.int32, (mine, SLOTS), 1).astype(jnp.float32)

    def choose(b, carry):
        before, base, index, was = carry
        here = pl.ds(pl.multiple_of(b * mine, mine), mine)
        after = before + total[here, :]
        passed = jnp.where(after <= slot, 1.0, 0.0)
        chosen[here, :] = was - passed
        return after, jnp.where(after <= slot, after, base), index + passed, passed

    zero = jnp.zeros((mine, SLOTS), jnp.float32)
    found, base, index, _ = lax.fori_loop(
        0, groups * blocks, choose, (zero, zero, zero, zero + 1.0), unroll=8
    )
    rest = slot - base

    out = []
    for q in range(mine):
        every = pl.ds(q, groups * blocks, stride=mine)
        picked = lax.dot_general(
            running[every, :].astype(jnp.bfloat16),
            chosen[every, :].astype(jnp.bfloat16),
            (((0,), (0,)), ((), ())),
            preferred_element_type=jnp.float32,
        )
        below = jnp.where(picked <= rest[q : q + 1, :], 1.0, 0.0)
        out.append(jnp.sum(below, axis=0, keepdims=True))
    inside = jnp.concatenate(out, axis=0)
    ids_ref[...] = jnp.where(slot < found, index * LANES + inside, -1.0).astype(jnp.int32)
    count_ref[...] = jnp.sum(
        jnp.where(diagonal, found[:, :mine], 0.0), axis=0, keepdims=True
    ).astype(jnp.int32)

    def drain(step, carry):
        source = flip(db, step, groups)

        @pl.when(step > 0)
        def _():
            code_copy(step).wait_send()

        near_copy(source).wait_send()
        far_copy(source).wait_send()
        return carry

    lax.fori_loop(0, groups, drain, 0)


def emit(ids_in, count_in, ids_ref, count_ref, sem):
    ids = pltpu.make_async_copy(ids_in, ids_ref, sem.at[0])
    count = pltpu.make_async_copy(count_in, count_ref, sem.at[1])
    ids.start()
    count.start()
    ids.wait()
    count.wait()


def per_device(groups, parts, codes, tables, limits):
    assert parts == 4 and groups & (groups - 1) == 0
    rows, width = codes.shape
    queries = tables.shape[0]
    mine = queries // parts
    blocks = groups * rows // LANES
    assert 2 * width * 128 <= 2 ** (BITS - 10)
    held = [
        pltpu.with_memory_space_constraint(array, pltpu.HBM)
        for array in (codes.T, tables, limits[None, :])
    ]
    ids, counts = pl.pallas_call(
        functools.partial(kernel, groups, parts),
        out_shape=(
            jax.ShapeDtypeStruct((mine, SLOTS), jnp.int32),
            jax.ShapeDtypeStruct((1, mine), jnp.int32),
        ),
        in_specs=[pl.BlockSpec(memory_space=pl.ANY)] * 3,
        out_specs=[pl.BlockSpec(memory_space=pltpu.VMEM)] * 2,
        scratch_shapes=[
            pltpu.VMEM((width, rows), jnp.int32),
            pltpu.VMEM(tables.shape, jnp.bfloat16),
            pltpu.VMEM((1, limits.shape[0]), jnp.int32),
            pltpu.VMEM((groups, width, rows), jnp.bfloat16),
            pltpu.VMEM((width, queries, K), jnp.bfloat16),
            pltpu.VMEM((groups, 2, 2, mine, rows), jnp.float32),
            pltpu.VMEM((groups, 2, mine, rows), jnp.float32),
            pltpu.VMEM((groups, 3, mine, rows // 4), jnp.int32),
            pltpu.VMEM((groups, 3, mine, rows // 4), jnp.int32),
            pltpu.VMEM((blocks * mine, LANES), jnp.float32),
            pltpu.VMEM((blocks * mine, LANES), jnp.float32),
            pltpu.VMEM((blocks * mine, LANES), jnp.float32),
            pltpu.SemaphoreType.DMA((3,)),
            pltpu.SemaphoreType.DMA((groups,)),
            pltpu.SemaphoreType.DMA((groups,)),
            pltpu.SemaphoreType.DMA((groups,)),
            pltpu.SemaphoreType.DMA((groups,)),
            pltpu.SemaphoreType.DMA((groups,)),
            pltpu.SemaphoreType.DMA((groups,)),
        ],
        compiler_params=pltpu.CompilerParams(
            collective_id=0, has_side_effects=True, vmem_limit_bytes=48 * 1024 * 1024
        ),
        name="retrieve",
    )(*held)

    ids, counts = pl.pallas_call(
        emit,
        out_shape=(
            jax.ShapeDtypeStruct((mine, SLOTS), jnp.int32),
            jax.ShapeDtypeStruct((1, mine), jnp.int32),
        ),
        in_specs=[pl.BlockSpec(memory_space=pl.ANY)] * 2,
        out_specs=[pl.BlockSpec(memory_space=pltpu.HBM)] * 2,
        scratch_shapes=[pltpu.SemaphoreType.DMA((2,))],
        compiler_params=pltpu.CompilerParams(vmem_limit_bytes=1024 * 1024),
        name="emit",
    )(ids, counts)
    return ids, counts[0]


def solution(mesh):
    placed = (P("db", "sub"), P("db", "sub", None), P())
    return jax.shard_map(
        functools.partial(per_device, mesh.shape["db"], mesh.shape["sub"]),
        mesh=mesh,
        in_specs=placed,
        out_specs=(P(("db", "sub"), None), P(("db", "sub"))),
        check_vma=False,
    )
```
